256 devices in a mesh: gz: 64 (over z, x, core), col: 4 (over y).
Axes of the slice: x: 4, y: 4, z: 8, core: 2. Of those that a mesh axis runs over, the one named last changes fastest.
Arguments:
- source: float32 [4096, 2048], P('gz', 'col'), may hold values from -6 to 6
- z_vectors: float32 [4096, 4096], P('gz', 'col'), may hold values from -0.25 to 0.25
- x_vectors: float32 [4, 4], replicated, may hold values from -3 to 3
- y_vectors: float32 [512, 512], replicated, may hold values from -0.25 to 0.25
- z_values: float32 [4096], replicated, may hold values from 0.1 to 3
- x_values: float32 [4], replicated, may hold values from 0.1 to 3
- y_values: float32 [512], replicated, may hold values from 0.1 to 3
Outputs:
- solution: float32 [4096, 2048], P('gz', 'col')
The draws below stay inside these ranges and needn't reach their ends.
All inputs are finite; a program needn't handle non-finite values.
Results may differ from the reference program's by a relative error of at most 0.000092.
Values sent between devices are 32-bit elements; how exact they have to be, the bound alone decides.
A program may use at most 64 MiB of HBM per device.

```python
import math
import jax
import jax.numpy as jnp
from jax import lax

NY = 512
NZ = 4096
NX = 4


def strengthened(drawn, own_key, source, target, blocks, factor):
    owner, partner = [(jnp.arange(drawn.shape[dim]) // (drawn.shape[dim] // blocks)).reshape([-1 if axis == dim else 1 for axis in range(drawn.ndim)]) for dim in (source, target)]
    chosen = jax.random.permutation(own_key, blocks)[partner]
    strong = (owner == chosen) | (owner == (partner + blocks // 2) % blocks)
    return jnp.where(strong, factor * drawn, drawn)


def level_of(stream_key, extent, split, low, top_value):
    def one(dim, blocks):
        draws = jax.random.uniform(jax.random.fold_in(jax.random.fold_in(stream_key, 6), dim), (blocks,), jnp.float32, low / len(split), top_value / len(split))
        return jnp.repeat(jnp.exp(draws), extent[dim] // blocks).reshape((-1,) + (1,) * (len(extent) - dim - 1))

    level = one(*split[0])
    for cut in split[1:]:
        level = level * one(*cut)
    return level


def gaussian(rng, extent, width, reach, split=(), held_as=jnp.bfloat16):
    factor_of = level_of(rng, extent, split, -0.22, 0.18) if split else 1.0
    entries = jax.random.normal(rng, extent, jnp.float32) * width * factor_of
    return jnp.minimum(jnp.maximum(entries, -reach), reach).astype(held_as)


def noise_with(own_key, dims, spread, most, cuts, heavy, held_as=jnp.bfloat16):
    values = spread * jax.random.normal(own_key, dims, jnp.float32)
    if cuts:
        values = values * level_of(own_key, dims, cuts, -0.22, 0.18)
    return jnp.clip(strengthened(values, jax.random.fold_in(own_key, 3), *heavy), -most, most).astype(held_as)


def setup_inputs(seed: int = 0) -> dict:
    splits = jax.random.split(jax.random.key(seed), 8)
    source = gaussian(splits[0], (NZ, NX * NY), 1.0, 6.0, ((0, 64), (1, 4)), jnp.float32)
    z_vectors = noise_with(splits[1], (NZ, NZ), NZ ** -0.5, 0.25, ((0, 64), (1, 4)), (0, 1, 64, 4.0), jnp.float32)
    x_vectors = gaussian(splits[2], (NX, NX), NX ** -0.5, 3.0, (), jnp.float32)
    y_vectors = gaussian(splits[3], (NY, NY), NY ** -0.5, 0.25, (), jnp.float32)
    z_values = jnp.clip(jnp.exp(jax.random.uniform(splits[4], (NZ,), jnp.float32, math.log(0.1), math.log(3.0))), 0.1, 3.0)
    x_values = jnp.clip(jnp.exp(jax.random.uniform(splits[5], (NX,), jnp.float32, math.log(0.1), math.log(3.0))), 0.1, 3.0)
    y_values = jnp.clip(jnp.exp(jax.random.uniform(splits[6], (NY,), jnp.float32, math.log(0.1), math.log(3.0))), 0.1, 3.0)
    return dict(source=source, z_vectors=z_vectors, x_vectors=x_vectors, y_vectors=y_vectors, z_values=z_values, x_values=x_values, y_values=y_values)


def reference(source, z_vectors, x_vectors, y_vectors, z_values, x_values, y_values):
    exact_mode = lax.Precision.HIGHEST
    field = source.reshape(NZ, NX, NY)
    along_y = jnp.einsum("zxy,yj->zxj", field, y_vectors, precision=exact_mode)
    along_x = jnp.einsum("zxj,xi->zij", along_y, x_vectors, precision=exact_mode)
    flat_modes = along_x.reshape(NZ, NX * NY)
    coefficients = lax.dot_general(z_vectors, flat_modes, (((0,), (0,)), ((), ())), precision=exact_mode, preferred_element_type=jnp.float32)
    divisor = z_values[:, None, None] + x_values[None, :, None] + y_values[None, None, :]
    scaled = coefficients.reshape(NZ, NX, NY) / divisor
    back_z = jnp.dot(z_vectors, scaled.reshape(NZ, NX * NY), precision=exact_mode, preferred_element_type=jnp.float32)
    back_x = jnp.einsum("zij,xi->zxj", back_z.reshape(NZ, NX, NY), x_vectors, precision=exact_mode)
    solution = jnp.einsum("zxj,yj->zxy", back_x, y_vectors, precision=exact_mode)
    return solution.reshape(NZ, NX * NY)
```

```python
import functools

import jax
import jax.numpy as jnp
from jax import lax
from jax.experimental import pallas as pl
from jax.experimental.pallas import tpu as pltpu
from jax.sharding import Mesh
from jax.sharding import PartitionSpec as P

NZ, NX, NC, NY = 8, 4, 2, 4
CH = 4
EXACT = lax.Precision.HIGHEST
MESH = pl.DeviceIdType.MESH


def dot(a, b):
    return lax.dot_general(
        a, b, (((1,), (0,)), ((), ())), precision=EXACT, preferred_element_type=jnp.float32
    )


def dot_nt(a, b):
    return lax.dot_general(
        a, b, (((1,), (1,)), ((), ())), precision=EXACT, preferred_element_type=jnp.float32
    )


def swap_blocks(parts):
    shape = parts[0].shape
    block = lax.broadcasted_iota(jnp.int32, shape, len(shape) - 1) // 32
    out = []
    for q in range(4):
        total = parts[q] if False else None
        for m in range(4):
            shift = 32 * ((m - q) % 4)
            moved = parts[m] if shift == 0 else pltpu.roll(parts[m], shift, len(shape) - 1)
            total = moved if total is None else jnp.where(block == m, moved, total)
        out.append(total)
    return out


def kernel(
    src, zv, yv, zval, xv, xval, yval, out,
    zg, fp, fg, ft, cs, cr, st, ba, bp, br, op, orr,
    zs_s, zs_r, zd_s, zd_r, fa_s, fa_r, fy_s, fy_r,
    cs_s, cs_r, st_s, st_r, by_s, by_r, oz_s, oz_r,
):
    z = lax.axis_index("z")
    x = lax.axis_index("x")
    c = lax.axis_index("c")
    y = lax.axis_index("y")
    pc = 1 - c
    kw = zv.shape[1] // CH
    waits = []

    def send(src_ref, dst_ref, s_sem, r_sem, dev):
        cp = pltpu.make_async_remote_copy(
            src_ref=src_ref, dst_ref=dst_ref, send_sem=s_sem, recv_sem=r_sem,
            device_id=dev, device_id_type=MESH,
        )
        cp.start()
        waits.append(cp)

    def await_recv(ref, sem):
        pltpu.make_async_remote_copy(
            src_ref=ref, dst_ref=ref, send_sem=sem, recv_sem=sem,
            device_id={"c": pc}, device_id_type=MESH,
        ).wait_recv()

    def zmod(k):
        return lax.rem(z + k + NZ, NZ)

    barrier = pltpu.get_barrier_semaphore()
    pl.semaphore_signal(barrier, inc=1, device_id={"c": pc}, device_id_type=MESH)
    for k in range(1, NZ):
        pl.semaphore_signal(barrier, inc=1, device_id={"z": zmod(k)}, device_id_type=MESH)
        pl.semaphore_signal(barrier, inc=1, device_id={"z": zmod(k), "c": pc}, device_id_type=MESH)
    for k in range(1, NX):
        pl.semaphore_signal(barrier, inc=1, device_id={"x": lax.rem(x + k, NX)}, device_id_type=MESH)
    for k in range(1, NY):
        pl.semaphore_signal(barrier, inc=1, device_id={"y": lax.rem(y + k, NY)}, device_id_type=MESH)

    along = dot(src[...], yv[...])
    for g in range(4):
        v = along[:, 128 * g : 128 * (g + 1)]
        pieces = swap_blocks([v[16 * m : 16 * (m + 1)] for m in range(4)])
        for q in range(4):
            fp[4 * g + q] = pieces[q]
    zg[c, z] = zv[...]
    fg[y, c, z] = fp[2 * z + c]

    pl.semaphore_wait(barrier, 1 + 2 * (NZ - 1) + (NX - 1) + (NY - 1))

    for k in (4, 3, 5, 2, 6, 1, 7):
        zz = zmod(k)
        for o in range(NC):
            cc = c if o == 0 else pc
            send(fp.at[2 * zz + cc], fg.at[y, c, z], fa_s.at[o, k], fa_r.at[o, k], {"z": zz, "c": cc})
    send(fp.at[2 * z + pc], fg.at[y, c, z], fa_s.at[1, 0], fa_r.at[1, 0], {"c": pc})

    def cols(ch):
        return pl.ds(ch * kw, kw)

    def ring_on(ch, s, way):
        zz = zmod(-s * way)
        block = zv.at[:, cols(ch)] if s == 0 else zg.at[c, zz, :, cols(ch)]
        w = 0 if way == 1 else 1
        send(block, zg.at[c, zz, :, cols(ch)], zs_s.at[w, s, ch], zs_r.at[w, s + 1, ch], {"z": zmod(way)})

    def to_partner(ch, s, way):
        zz = zmod(-s * way)
        block = zv.at[:, cols(ch)] if s == 0 else zg.at[c, zz, :, cols(ch)]
        w = 0 if way == 1 else 1
        send(block, zg.at[c, zz, :, cols(ch)], zd_s.at[w, s, ch], zd_r.at[w, s, ch], {"c": pc})

    def own(ch):
        ring_on(ch, 0, 1)
        ring_on(ch, 0, -1)
        to_partner(ch, 0, 1)

    def arrival(s, ch):
        for way in (1, -1):
            w = 0 if way == 1 else 1
            if s == NZ // 2 and (ch % 2 == 0) != (way == 1):
                continue
            await_recv(zg.at[c, zmod(-s * way), :, cols(ch)], zs_r.at[w, s, ch])
            if s + 1 < NZ // 2 or (s + 1 == NZ // 2 and (ch % 2 == 0) == (way == 1)):
                ring_on(ch, s, way)
            to_partner(ch, s, way)

    def partner_arrivals(ch):
        await_recv(zg.at[pc, z, :, cols(ch)], zd_r.at[0, 0, ch])
        for s in range(1, NZ // 2 + 1):
            for way in (1, -1):
                w = 0 if way == 1 else 1
                if s == NZ // 2 and (ch % 2 == 0) != (way == 1):
                    continue
                await_recv(zg.at[pc, zmod(-s * way), :, cols(ch)], zd_r.at[w, s, ch])

    def f_over_y():
        for k in range(1, NZ):
            zz = zmod(-k)
            for o in range(NC):
                cc = c if o == 0 else pc
                await_recv(fg.at[y, cc, zz], fa_r.at[o, k])
        await_recv(fg.at[y, pc, z], fa_r.at[1, 0])
        for k in (2, 1, 3):
            send(fg.at[y], fg.at[y], fy_s.at[k], fy_r.at[k], {"y": lax.rem(y + k, NY)})

    def f_turned():
        for k in range(1, NY):
            await_recv(fg.at[lax.rem(y - k + NY, NY)], fy_r.at[k])
        for pair in range(NC * NZ // 2):
            rows = []
            for b in (2 * pair, 2 * pair + 1):
                rows += swap_blocks([fg[p, b // NZ, b % NZ] for p in range(NY)])
            ft[:, 128 * pair : 128 * (pair + 1)] = jnp.concatenate(rows, axis=0).T

    def z_chunk(ch):
        return zg[:, :, :, ch * kw : (ch + 1) * kw].reshape(NC * NZ * 64, kw)

    def coefficients(ch):
        partner_arrivals(ch)
        part = dot(ft[...], z_chunk(ch))
        cs[ch] = part.reshape(4, NX, 8, kw)
        for k in (2, 1, 3):
            xx = lax.rem(x + k, NX)
            send(cs.at[ch, :, xx], cr.at[ch, k], cs_s.at[ch, k], cs_r.at[ch, k], {"x": xx})

    def scale(ch):
        total = cs[ch, :, x]
        for k in range(1, NX):
            await_recv(cr.at[ch, k], cs_r.at[ch, k])
            total = total + cr[ch, k]
        base = (2 * z + c) * 32 + 8 * x
        row = lax.broadcasted_iota(jnp.int32, (8, kw), 0)
        yvals = jnp.zeros((8, kw), jnp.float32)
        for t in range(8):
            yvals = jnp.where(row == t, yval[base + t], yvals)
        zy = yvals + zval[:, pl.ds(pl.multiple_of(y * zv.shape[1] + ch * kw, 128), kw)]
        scaled = []
        for i in range(4):
            mode = xv[0, i] * total[0]
            for p in range(1, 4):
                mode = mode + xv[p, i] * total[p]
            scaled.append(mode / (zy + xval[i]))
        for p in range(4):
            back = xv[p, 0] * scaled[0]
            for i in range(1, 4):
                back = back + xv[p, i] * scaled[i]
            st[ch, p, x] = back
        for k in (2, 1, 3):
            send(st.at[ch, :, x], st.at[ch, :, x], st_s.at[ch, k], st_r.at[ch, k], {"x": lax.rem(x + k, NX)})

    def scaled_all(ch):
        for k in range(1, NX):
            await_recv(st.at[ch, :, lax.rem(x - k + NX, NX)], st_r.at[ch, k])

    def back_z(ch):
        scaled_all(ch)
        part = dot_nt(z_chunk(ch), st[ch].reshape(128, kw))
        if ch == 0:
            ba[...] = part
        else:
            ba[...] += part

    own(0)
    own(1)
    arrival(1, 0)
    arrival(1, 1)
    f_over_y()
    arrival(2, 0)
    own(2)
    arrival(2, 1)
    own(3)
    arrival(3, 0)
    arrival(3, 1)
    arrival(1, 2)
    arrival(1, 3)
    f_turned()
    arrival(4, 0)
    arrival(4, 1)
    arrival(2, 2)
    arrival(2, 3)
    coefficients(0)
    coefficients(1)
    arrival(3, 2)
    arrival(3, 3)
    scale(0)
    scale(1)
    arrival(4, 2)
    arrival(4, 3)
    coefficients(2)
    back_z(0)
    coefficients(3)
    back_z(1)
    scale(2)
    scale(3)
    back_z(2)
    back_z(3)

    half = NZ // 2
    for cc in range(NC):
        for h in range(2):
            for b in range(half):
                at = (cc * NZ + h * half + b) * 64
                pieces = swap_blocks([ba[at + 16 * m : at + 16 * (m + 1), :] for m in range(4)])
                for p in range(NY):
                    bp[p, cc, h * half + b] = pieces[p]
            for k in (2, 1, 3):
                yy = lax.rem(y + k, NY)
                send(
                    bp.at[yy, cc, pl.ds(h * half, half)], br.at[k, cc, pl.ds(h * half, half)],
                    by_s.at[cc, h, k], by_r.at[cc, h, k], {"y": yy},
                )
    for cc in range(NC):
        for h in range(2):
            part = pl.ds(h * half, half)
            total = bp[y, cc, part]
            for k in range(1, NY):
                await_recv(br.at[k, cc, part], by_r.at[cc, h, k])
                total = total + br[k, cc, part]
            op[cc, part] = total
    for k in (4, 3, 5, 2, 6, 1, 7):
        zz = zmod(k)
        for o in range(NC):
            cc = c if o == 0 else pc
            send(op.at[cc, zz], orr.at[2 * z + c], oz_s.at[o, k], oz_r.at[o, k], {"z": zz, "c": cc})
    send(op.at[pc, z], orr.at[2 * z + c], oz_s.at[1, 0], oz_r.at[1, 0], {"c": pc})
    orr[2 * z + c] = op[c, z]
    for k in range(1, NZ):
        zz = zmod(-k)
        for o in range(NC):
            cc = c if o == 0 else pc
            await_recv(orr.at[2 * zz + cc], oz_r.at[o, k])
    await_recv(orr.at[2 * z + pc], oz_r.at[1, 0])
    lanes = []
    for g in range(4):
        lanes.append(jnp.concatenate(swap_blocks([orr[4 * g + q] for q in range(4)]), axis=0))
    out[...] = dot_nt(jnp.concatenate(lanes, axis=1), yv[...])

    for cp in waits:
        cp.wait_send()


def shards(source, z_vectors, x_vectors, y_vectors, z_values, x_values, y_values):
    f32 = jnp.float32
    dma = pltpu.SemaphoreType.DMA
    vmem = pl.BlockSpec(memory_space=pltpu.VMEM)
    smem = pl.BlockSpec(memory_space=pltpu.SMEM)
    kw = z_vectors.shape[1] // CH
    return pl.pallas_call(
        kernel,
        out_shape=jax.ShapeDtypeStruct(source.shape, f32),
        in_specs=[vmem, vmem, vmem, vmem, smem, smem, smem],
        out_specs=vmem,
        scratch_shapes=[
            pltpu.VMEM((NC, NZ, 64, z_vectors.shape[1]), f32),
            pltpu.VMEM((16, 16, 128), f32),
            pltpu.VMEM((NY, NC, NZ, 16, 128), f32),
            pltpu.VMEM((128, 1024), f32),
            pltpu.VMEM((CH, 4, NX, 8, kw), f32),
            pltpu.VMEM((CH, NX, 4, 8, kw), f32),
            pltpu.VMEM((CH, 4, NX, 8, kw), f32),
            pltpu.VMEM((1024, 128), f32),
            pltpu.VMEM((NY, NC, NZ, 16, 128), f32),
            pltpu.VMEM((NY, NC, NZ, 16, 128), f32),
            pltpu.VMEM((NC, NZ, 16, 128), f32),
            pltpu.VMEM((16, 16, 128), f32),
            dma((2, 5, CH)), dma((2, 5, CH)), dma((2, 5, CH)), dma((2, 5, CH)),
            dma((2, NZ)), dma((2, NZ)), dma((NY,)), dma((NY,)),
            dma((CH, NX)), dma((CH, NX)), dma((CH, NX)), dma((CH, NX)),
            dma((2, 2, NY)), dma((2, 2, NY)), dma((2, NZ)), dma((2, NZ)),
        ],
        compiler_params=pltpu.CompilerParams(
            collective_id=0, has_side_effects=True, vmem_limit_bytes=48 * 1024 * 1024
        ),
    )(source, z_vectors, y_vectors, z_values.reshape(1, -1), x_vectors, x_values, y_values)


def solution(mesh):
    torus = Mesh(mesh.devices.reshape(NZ, NX, NC, NY), ("z", "x", "c", "y"))
    rows = ("z", "x", "c")
    return jax.shard_map(
        shards,
        mesh=torus,
        in_specs=(P(rows, "y"), P(rows, "y"), P(), P(), P(), P(), P()),
        out_specs=P(rows, "y"),
        check_vma=False,
    )
```

```python
import jax
import jax.numpy as jnp
from jax import lax
from jax.experimental import pallas as pl
from jax.experimental.pallas import tpu as pltpu
from jax.sharding import Mesh
from jax.sharding import PartitionSpec as P

NZ, NX, NC, NY = 8, 4, 2, 4
MESH = pl.DeviceIdType.MESH
WIDTHS = (128, 256, 128, 128, 256, 128)
N = len(WIDTHS)
LAST = 3
STARTS = tuple(sum(WIDTHS[:ch]) for ch in range(N))
GROUPS = ((4, 3), (5, 2), (6, 1), (7, 0))


def dot_exact(a, b):
    return lax.dot_general(
        a, b, (((1,), (0,)), ((), ())),
        precision=lax.Precision.HIGHEST, preferred_element_type=jnp.float32,
    )


def dot(a, b, b_dim=0):
    return lax.dot_general(a, b, (((1,), (b_dim,)), ((), ())), preferred_element_type=jnp.float32)


def halves(value):
    high = value.astype(jnp.bfloat16)
    return high, (value - high.astype(jnp.float32)).astype(jnp.bfloat16)


def swap_blocks(parts):
    shape = parts[0].shape
    block = lax.broadcasted_iota(jnp.int32, shape, 1) // 32
    out = []
    for q in range(4):
        total = None
        for m in range(4):
            shift = 32 * ((m - q) % 4)
            moved = parts[m] if shift == 0 else pltpu.roll(parts[m], shift, 1)
            total = moved if total is None else jnp.where(block == m, moved, total)
        out.append(total)
    return out


def kernel(
    src_h, zv_h, yv_h, zval_h, xv_h, xval_h, yval_h, out,
    src, zv, yv, zval, xv, xval, yval, in_s,
    zg, zh, zl, yth, ytl, fp, fg, fts, cs, cr, st, ba, bp, br, op, orr,
    zs_s, zs_r, zd_s, zd_r, fa_s, fa_r, fy_s, fy_r,
    cs_s, cs_r, st_s, st_r, by_s, by_r, oz_s, oz_r,
):
    z = lax.axis_index("z")
    x = lax.axis_index("x")
    c = lax.axis_index("c")
    y = lax.axis_index("y")
    pc = 1 - c

    def send(src_ref, dst_ref, s_sem, r_sem, dev):
        pltpu.make_async_remote_copy(
            src_ref=src_ref, dst_ref=dst_ref, send_sem=s_sem, recv_sem=r_sem,
            device_id=dev, device_id_type=MESH,
        ).start()

    def sized(ref, sem):
        return pltpu.make_async_remote_copy(
            src_ref=ref, dst_ref=ref, send_sem=sem, recv_sem=sem,
            device_id={"c": pc}, device_id_type=MESH,
        )

    def received(ref, sem):
        sized(ref, sem).wait_recv()

    def sent(ref, sem):
        sized(ref, sem).wait_send()

    def zmod(k):
        return lax.rem(z + k + NZ, NZ)

    def core(o):
        return c if o == 0 else pc

    def cols(ch):
        return pl.ds(STARTS[ch], WIDTHS[ch])

    def load(n):
        pairs = [(zv_h, zv), (src_h, src), (yv_h, yv), (zval_h, zval), (xv_h, xv), (xval_h, xval), (yval_h, yval)]
        return pltpu.make_async_copy(*pairs[n], in_s.at[n])

    def start():
        for n in range(7):
            load(n).start()
        barrier = pltpu.get_barrier_semaphore()

        def greet(dev):
            pl.semaphore_signal(barrier, inc=1, device_id=dev, device_id_type=MESH)

        for k in (4, 3, 5, 2, 6, 1, 7):
            greet({"z": zmod(k)})
            greet({"z": zmod(k), "c": pc})
        for k in range(1, NX):
            greet({"x": lax.rem(x + k, NX)})
        for k in range(1, NY):
            greet({"y": lax.rem(y + k, NY)})
        greet({"c": pc})

    def along_y():
        load(1).wait()
        load(2).wait()
        along = dot_exact(src[...], yv[...])
        for g in range(4):
            v = along[:, 128 * g : 128 * (g + 1)]
            pieces = swap_blocks([v[16 * m : 16 * (m + 1)] for m in range(4)])
            for q in range(4):
                fp[4 * g + q] = pieces[q]
        fg[y, c, z] = fp[2 * z + c]

    def meet():
        load(0).wait()
        pl.semaphore_wait(pltpu.get_barrier_semaphore(), 1 + 2 * (NZ - 1) + (NX - 1) + (NY - 1))

    def pass_on(ch, s, way):
        slot = zmod(-s * way)
        block = zv.at[:, cols(ch)] if s == 0 else zg.at[c, slot, :, cols(ch)]
        if s < NZ // 2 - 1 or (s == NZ // 2 - 1 and (ch % 2 == 0) == (way == 1)):
            send(block, zg.at[c, slot, :, cols(ch)], zs_s, zs_r.at[s, ch], {"z": zmod(way)})
        if s > 0 or way == 1:
            send(block, zg.at[c, slot, :, cols(ch)], zd_s, zd_r.at[ch], {"c": pc})

    def own(ch):
        pass_on(ch, 0, 1)
        pass_on(ch, 0, -1)

    def arr(s, ch):
        ways = (1, -1) if s < NZ // 2 else ((1,) if ch % 2 == 0 else (-1,))
        received(zg.at[c, pl.ds(0, len(ways)), :, cols(ch)], zs_r.at[s - 1, ch])
        for way in ways:
            pass_on(ch, s, way)

    def prepare():
        zg[c, z] = zv[...]
        for n in range(3, 7):
            load(n).wait()
        high, low = halves(yv[...].T)
        yth[...] = high
        ytl[...] = low

    def a2a():
        for k in (4, 3, 5, 2, 6, 1, 7):
            for o in range(NC):
                dev = {"z": zmod(k), "c": core(o)}
                send(fp.at[2 * zmod(k) + core(o)], fg.at[y, c, z], fa_s, fa_r, dev)
        send(fp.at[2 * z + pc], fg.at[y, c, z], fa_s, fa_r, {"c": pc})

    def fy():
        received(fp.at[pl.ds(0, 15)], fa_r)
        for k in (2, 1, 3):
            send(fg.at[y], fg.at[y], fy_s, fy_r, {"y": lax.rem(y + k, NY)})

    def ft():
        received(fg.at[pl.ds(0, NY - 1)], fy_r)
        for pair in range(NC * NZ // 2):
            rows = []
            for b in (2 * pair, 2 * pair + 1):
                rows += swap_blocks([fg[p, b // NZ, b % NZ] for p in range(NY)])
            high, low = halves(jnp.concatenate(rows, axis=0).T)
            fts[0:128, 128 * pair : 128 * (pair + 1)] = high
            fts[128:256, 128 * pair : 128 * (pair + 1)] = low

    def C(ch):
        lo, hi = STARTS[ch], STARTS[ch] + WIDTHS[ch]
        received(zg.at[pc, :, :, cols(ch)], zd_r.at[ch])
        high, low = halves(zg[:, :, :, lo:hi].reshape(NC * NZ * 64, WIDTHS[ch]))
        zh[:, lo:hi] = high
        zl[:, lo:hi] = low
        both = dot(fts[...], high)
        part = both[:128] + both[128:] + dot(fts[:128], low)
        cs[:, :, :, lo:hi] = part.reshape(4, NX, 8, WIDTHS[ch])
        for k in (2, 1, 3):
            xx = lax.rem(x + k, NX)
            send(cs.at[:, xx, :, cols(ch)], cr.at[k - 1, :, :, cols(ch)], cs_s, cs_r.at[ch], {"x": xx})

    def S(ch):
        lo, hi = STARTS[ch], STARTS[ch] + WIDTHS[ch]
        received(cr.at[:, :, :, cols(ch)], cs_r.at[ch])
        base = (2 * z + c) * 32 + 8 * x
        row = lax.broadcasted_iota(jnp.int32, (8, WIDTHS[ch]), 0)
        yvals = jnp.zeros((8, WIDTHS[ch]), jnp.float32)
        for t in range(8):
            yvals = jnp.where(row == t, yval[base + t], yvals)
        zy = yvals + zval[:, pl.ds(pl.multiple_of(y * zv.shape[1] + lo, 128), WIDTHS[ch])]
        total = [
            cs[p, x, :, lo:hi] + cr[0, p, :, lo:hi] + cr[1, p, :, lo:hi] + cr[2, p, :, lo:hi] for p in range(4)
        ]
        scaled = []
        for i in range(4):
            mode = xv[0, i] * total[0]
            for p in range(1, 4):
                mode = mode + xv[p, i] * total[p]
            scaled.append(mode / (zy + xval[i]))
        for p in range(4):
            back = xv[p, 0] * scaled[0]
            for i in range(1, 4):
                back = back + xv[p, i] * scaled[i]
            st[p, x, :, lo:hi] = back
        for k in (2, 1, 3):
            piece = st.at[:, x, :, cols(ch)]
            send(piece, piece, st_s, st_r.at[ch], {"x": lax.rem(x + k, NX)})

    def modes_back(high, low, ch):
        lo, hi = STARTS[ch], STARTS[ch] + WIDTHS[ch]
        s_high, s_low = halves(st[:, :, :, lo:hi].reshape(128, WIDTHS[ch]))
        both = dot(high, jnp.concatenate([s_high, s_low], axis=0), 1)
        return both[:, :128] + both[:, 128:] + dot(low, s_high, 1)

    def B(ch):
        lo, hi = STARTS[ch], STARTS[ch] + WIDTHS[ch]
        received(st.at[:, pl.ds(0, NX - 1), :, cols(ch)], st_r.at[ch])
        if ch == LAST:
            return
        part = modes_back(zh[:, lo:hi], zl[:, lo:hi], ch)
        if ch == 0:
            ba[...] = part
        else:
            ba[...] += part

    def blocks(g):
        return [(k, o, (core(o) * NZ + zmod(k)) * 64) for k in GROUPS[g] for o in range(NC)]

    def over_y(g):
        lo, hi = STARTS[LAST], STARTS[LAST] + WIDTHS[LAST]

        def rows(ref, a, b):
            return jnp.concatenate(
                [ref[pl.ds(pl.multiple_of(at, 64), 64), a:b] for _, _, at in blocks(g)], axis=0
            )

        total = rows(ba, 0, 128) + modes_back(rows(zh, lo, hi), rows(zl, lo, hi), LAST)
        for n in range(4):
            pieces = swap_blocks([total[64 * n + 16 * m : 64 * n + 16 * (m + 1)] for m in range(4)])
            for p in range(NY):
                bp[p, g, n] = pieces[p]
        for k in (2, 1, 3):
            yy = lax.rem(y + k, NY)
            send(bp.at[yy, g], br.at[k - 1, g], by_s, by_r.at[g], {"y": yy})

    def leave(g):
        received(br.at[:, g], by_r.at[g])
        op[g] = bp[y, g] + br[0, g] + br[1, g] + br[2, g]
        for n, (k, o, _) in enumerate(blocks(g)):
            if k == 0 and o == 0:
                orr[2 * z + c] = op[g, n]
            else:
                send(op.at[g, n], orr.at[2 * z + c], oz_s, oz_r, {"z": zmod(k), "c": core(o)})

    def finish():
        received(orr.at[pl.ds(0, 15)], oz_r)
        lanes = []
        for g in range(4):
            lanes.append(jnp.concatenate(swap_blocks([orr[4 * g + q] for q in range(4)]), axis=0))
        high, low = halves(jnp.concatenate(lanes, axis=1))
        both = dot(jnp.concatenate([high, low], axis=0), yth[...])
        out[...] = both[:64] + both[64:] + dot(high, ytl[...])

    def drain():
        sent(zg.at[0, pl.ds(0, NZ - 1)], zs_s)
        sent(zg.at[0], zd_s)
        sent(fp.at[pl.ds(0, 15)], fa_s)
        sent(fg.at[pl.ds(0, NY - 1)], fy_s)
        sent(cr, cs_s)
        sent(st.at[:, pl.ds(0, NX - 1)], st_s)
        sent(br, by_s)
        sent(orr.at[pl.ds(0, 15)], oz_s)

    plan = [
        (start,), (along_y,), (meet,),
        (own, 0), (own, 1), (prepare,), (a2a,), (arr, 1, 0), (own, 4), (arr, 1, 1), (arr, 2, 0), (fy,),
        (own, 2), (arr, 1, 4), (arr, 2, 1), (own, 5), (arr, 3, 0), (own, 3), (arr, 1, 2), (arr, 2, 4),
        (arr, 3, 1), (arr, 1, 5), (ft,), (arr, 4, 0), (arr, 1, 3), (arr, 2, 2), (C, 0), (arr, 3, 4),
        (arr, 4, 1), (arr, 2, 5), (C, 1), (arr, 2, 3), (arr, 3, 2), (S, 0), (arr, 4, 4), (arr, 3, 5), (C, 4),
        (arr, 3, 3), (arr, 4, 2), (S, 1), (arr, 4, 5), (C, 2), (B, 0), (arr, 4, 3), (C, 5), (C, 3), (S, 4),
        (B, 1), (S, 2), (S, 5), (S, 3), (B, 4), (B, 2), (B, 5), (B, 3),
        (over_y, 0), (over_y, 1), (over_y, 2), (over_y, 3),
        (leave, 0), (leave, 1), (leave, 2), (leave, 3),
        (finish,), (drain,),
    ]
    for step, *args in plan:
        with jax.named_scope("_".join([step.__name__, *map(str, args)])):
            step(*args)


def shards(source, z_vectors, x_vectors, y_vectors, z_values, x_values, y_values):
    f32, bf16 = jnp.float32, jnp.bfloat16
    vmem, smem, dma = pltpu.VMEM, pltpu.SMEM, pltpu.SemaphoreType.DMA
    modes = z_vectors.shape[1]
    one = dma(())
    return pl.pallas_call(
        kernel,
        out_shape=jax.ShapeDtypeStruct(source.shape, f32),
        in_specs=[pl.BlockSpec(memory_space=pl.ANY)] * 7,
        out_specs=pl.BlockSpec(memory_space=pltpu.VMEM),
        scratch_shapes=[
            vmem(source.shape, f32),
            vmem(z_vectors.shape, f32),
            vmem(y_vectors.shape, f32),
            vmem((1, z_values.shape[0]), f32),
            smem(x_vectors.shape, f32),
            smem(x_values.shape, f32),
            smem(y_values.shape, f32),
            dma((7,)),
            vmem((NC, NZ, 64, modes), f32),
            vmem((1024, modes), bf16),
            vmem((1024, modes), bf16),
            vmem((512, 512), bf16),
            vmem((512, 512), bf16),
            vmem((16, 16, 128), f32),
            vmem((NY, NC, NZ, 16, 128), f32),
            vmem((256, 1024), bf16),
            vmem((4, NX, 8, modes), f32),
            vmem((NX - 1, 4, 8, modes), f32),
            vmem((4, NX, 8, modes), f32),
            vmem((1024, 128), f32),
            vmem((NY, 4, 4, 16, 128), f32),
            vmem((NY - 1, 4, 4, 16, 128), f32),
            vmem((4, 4, 16, 128), f32),
            vmem((16, 16, 128), f32),
            one, dma((4, N)), one, dma((N,)), one, one, one, one,
            one, dma((N,)), one, dma((N,)), one, dma((4,)), one, one,
        ],
        compiler_params=pltpu.CompilerParams(
            collective_id=0, has_side_effects=True, vmem_limit_bytes=67_043_328
        ),
    )(source, z_vectors, y_vectors, z_values.reshape(1, -1), x_vectors, x_values, y_values)


def solution(mesh):
    torus = Mesh(mesh.devices.reshape(NZ, NX, NC, NY), ("z", "x", "c", "y"))
    rows = ("z", "x", "c")
    return jax.shard_map(
        shards,
        mesh=torus,
        in_specs=(P(rows, "y"), P(rows, "y"), P(), P(), P(), P(), P()),
        out_specs=P(rows, "y"),
        check_vma=False,
    )
```

```python
import jax
import jax.numpy as jnp
from jax import lax
from jax.experimental import pallas as pl
from jax.experimental.pallas import tpu as pltpu
from jax.sharding import Mesh
from jax.sharding import PartitionSpec as P

NZ, NX, NC, NY = 8, 4, 2, 4
MESH = pl.DeviceIdType.MESH
WIDTHS = (128, 256, 128, 128, 256, 128)
N = len(WIDTHS)
LAST = 3
STARTS = tuple(sum(WIDTHS[:ch]) for ch in range(N))
GROUPS = ((4, 3), (5, 2), (6, 1), (7, 0))


def dot_exact(a, b):
    return lax.dot_general(
        a, b, (((1,), (0,)), ((), ())),
        precision=lax.Precision.HIGHEST, preferred_element_type=jnp.float32,
    )


def dot(a, b, b_dim=0):
    return lax.dot_general(a, b, (((1,), (b_dim,)), ((), ())), preferred_element_type=jnp.float32)


def halves(value):
    high = value.astype(jnp.bfloat16)
    return high, (value - high.astype(jnp.float32)).astype(jnp.bfloat16)


def swap_blocks(parts):
    shape = parts[0].shape
    block = lax.broadcasted_iota(jnp.int32, shape, 1) // 32
    out = []
    for q in range(4):
        total = None
        for m in range(4):
            shift = 32 * ((m - q) % 4)
            moved = parts[m] if shift == 0 else pltpu.roll(parts[m], shift, 1)
            total = moved if total is None else jnp.where(block == m, moved, total)
        out.append(total)
    return out


def kernel(
    src_h, zv_h, yv_h, zval_h, xv_h, xval_h, yval_h, out,
    src, zv, yv, zval, xv, xval, yval, in_s,
    zg, zh, zl, yth, ytl, fp, fg, fts, cs, cr, st, ba, bp, br, op, orr,
    zs_s, zs_r, zd_s, zd_r, fa_s, fa_r, fy_s, fy_r,
    cs_s, cs_r, st_s, st_r, by_s, by_r, oz_s, oz_r, zi, xi, yi, pi,
):
    z = lax.axis_index("z")
    x = lax.axis_index("x")
    c = lax.axis_index("c")
    y = lax.axis_index("y")
    pc = 1 - c

    def send(src_ref, dst_ref, s_sem, r_sem, dev):
        pltpu.make_async_remote_copy(
            src_ref=src_ref, dst_ref=dst_ref, send_sem=s_sem, recv_sem=r_sem,
            device_id=dev, device_id_type=MESH,
        ).start()

    def sized(ref, sem):
        return pltpu.make_async_remote_copy(
            src_ref=ref, dst_ref=ref, send_sem=sem, recv_sem=sem,
            device_id={"c": pc}, device_id_type=MESH,
        )

    def received(ref, sem):
        sized(ref, sem).wait_recv()

    def sent(ref, sem):
        sized(ref, sem).wait_send()

    def zmod(k):
        return lax.rem(z + k + NZ, NZ)

    def xmod(k):
        return lax.rem(x + k + NX, NX)

    def ymod(k):
        return lax.rem(y + k + NY, NY)

    def tell(sem, dev):
        pl.semaphore_signal(sem, inc=1, device_id=dev, device_id_type=MESH)

    def core(o):
        return c if o == 0 else pc

    def cols(ch):
        return pl.ds(STARTS[ch], WIDTHS[ch])

    def load(n):
        pairs = [(zv_h, zv), (src_h, src), (yv_h, yv), (zval_h, zval), (xv_h, xv), (xval_h, xval), (yval_h, yval)]
        return pltpu.make_async_copy(*pairs[n], in_s.at[n])

    def start():
        for n in range(7):
            load(n).start()
        for dev in (
            {"z": zmod(1)}, {"z": zmod(-1)}, {"x": xmod(1)}, {"x": xmod(-1)}, {"y": ymod(1)}, {"y": ymod(-1)}, {"c": pc}
        ):
            tell(pltpu.get_barrier_semaphore(), dev)

    def along_y():
        load(1).wait()
        load(2).wait()
        along = dot_exact(src[...], yv[...])
        for g in range(4):
            v = along[:, 128 * g : 128 * (g + 1)]
            pieces = swap_blocks([v[16 * m : 16 * (m + 1)] for m in range(4)])
            for q in range(4):
                fp[4 * g + q] = pieces[q]
        fg[y, c, z] = fp[2 * z + c]

    def meet():
        load(0).wait()
        pl.semaphore_wait(pltpu.get_barrier_semaphore(), 7)
        tell(zi.at[0, 0], {"z": zmod(1)})
        tell(zi.at[1, 0], {"z": zmod(-1)})
        tell(xi, {"x": xmod(-1)})
        tell(yi, {"y": ymod(-1)})

    def meet_far():
        pl.semaphore_wait(zi.at[0, 0], 1)
        tell(zi.at[0, 1], {"z": zmod(1)})
        pl.semaphore_wait(zi.at[1, 0], 1)
        tell(zi.at[1, 1], {"z": zmod(-1)})
        pl.semaphore_wait(zi.at[0, 1], 1)
        tell(zi.at[0, 2], {"z": zmod(1)})
        pl.semaphore_wait(zi.at[1, 1], 1)
        pl.semaphore_wait(xi, 1)
        pl.semaphore_wait(yi, 1)
        pl.semaphore_wait(zi.at[0, 2], 1)
        tell(pi, {"c": pc})
        pl.semaphore_wait(pi, 1)

    def pass_on(ch, s, way):
        slot = zmod(-s * way)
        block = zv.at[:, cols(ch)] if s == 0 else zg.at[c, slot, :, cols(ch)]
        if s < NZ // 2 - 1 or (s == NZ // 2 - 1 and (ch % 2 == 0) == (way == 1)):
            send(block, zg.at[c, slot, :, cols(ch)], zs_s, zs_r.at[s, ch], {"z": zmod(way)})
        if s > 0 or way == 1:
            send(block, zg.at[c, slot, :, cols(ch)], zd_s, zd_r.at[ch], {"c": pc})

    def own(ch):
        pass_on(ch, 0, 1)
        pass_on(ch, 0, -1)

    def arr(s, ch):
        ways = (1, -1) if s < NZ // 2 else ((1,) if ch % 2 == 0 else (-1,))
        received(zg.at[c, pl.ds(0, len(ways)), :, cols(ch)], zs_r.at[s - 1, ch])
        for way in ways:
            pass_on(ch, s, way)

    def prepare():
        zg[c, z] = zv[...]
        for n in range(3, 7):
            load(n).wait()
        high, low = halves(yv[...].T)
        yth[...] = high
        ytl[...] = low

    def a2a():
        for k in (4, 3, 5, 2, 6, 1, 7):
            for o in range(NC):
                dev = {"z": zmod(k), "c": core(o)}
                send(fp.at[2 * zmod(k) + core(o)], fg.at[y, c, z], fa_s, fa_r, dev)
        send(fp.at[2 * z + pc], fg.at[y, c, z], fa_s, fa_r, {"c": pc})

    def fy():
        received(fp.at[pl.ds(0, 15)], fa_r)
        for k in (2, 1, 3):
            send(fg.at[y], fg.at[y], fy_s, fy_r, {"y": ymod(k)})

    def ft():
        received(fg.at[pl.ds(0, NY - 1)], fy_r)
        for pair in range(NC * NZ // 2):
            rows = []
            for b in (2 * pair, 2 * pair + 1):
                rows += swap_blocks([fg[p, b // NZ, b % NZ] for p in range(NY)])
            high, low = halves(jnp.concatenate(rows, axis=0).T)
            fts[0:128, 128 * pair : 128 * (pair + 1)] = high
            fts[128:256, 128 * pair : 128 * (pair + 1)] = low

    def C(ch):
        lo, hi = STARTS[ch], STARTS[ch] + WIDTHS[ch]
        received(zg.at[pc, :, :, cols(ch)], zd_r.at[ch])
        high, low = halves(zg[:, :, :, lo:hi].reshape(NC * NZ * 64, WIDTHS[ch]))
        zh[:, lo:hi] = high
        zl[:, lo:hi] = low
        both = dot(fts[...], high)
        part = both[:128] + both[128:] + dot(fts[:128], low)
        cs[:, :, :, lo:hi] = part.reshape(4, NX, 8, WIDTHS[ch])
        for k in (2, 1, 3):
            xx = xmod(k)
            send(cs.at[:, xx, :, cols(ch)], cr.at[k - 1, :, :, cols(ch)], cs_s, cs_r.at[ch], {"x": xx})

    def S(ch):
        lo, hi = STARTS[ch], STARTS[ch] + WIDTHS[ch]
        received(cr.at[:, :, :, cols(ch)], cs_r.at[ch])
        base = (2 * z + c) * 32 + 8 * x
        row = lax.broadcasted_iota(jnp.int32, (8, WIDTHS[ch]), 0)
        yvals = jnp.zeros((8, WIDTHS[ch]), jnp.float32)
        for t in range(8):
            yvals = jnp.where(row == t, yval[base + t], yvals)
        zy = yvals + zval[:, pl.ds(pl.multiple_of(y * zv.shape[1] + lo, 128), WIDTHS[ch])]
        total = [
            cs[p, x, :, lo:hi] + cr[0, p, :, lo:hi] + cr[1, p, :, lo:hi] + cr[2, p, :, lo:hi] for p in range(4)
        ]
        scaled = []
        for i in range(4):
            mode = xv[0, i] * total[0]
            for p in range(1, 4):
                mode = mode + xv[p, i] * total[p]
            scaled.append(mode / (zy + xval[i]))
        for p in range(4):
            back = xv[p, 0] * scaled[0]
            for i in range(1, 4):
                back = back + xv[p, i] * scaled[i]
            st[p, x, :, lo:hi] = back
        for k in (2, 1, 3):
            piece = st.at[:, x, :, cols(ch)]
            send(piece, piece, st_s, st_r.at[ch], {"x": xmod(k)})

    def modes_back(high, low, ch):
        lo, hi = STARTS[ch], STARTS[ch] + WIDTHS[ch]
        s_high, s_low = halves(st[:, :, :, lo:hi].reshape(128, WIDTHS[ch]))
        both = dot(high, jnp.concatenate([s_high, s_low], axis=0), 1)
        return both[:, :128] + both[:, 128:] + dot(low, s_high, 1)

    def B(ch):
        lo, hi = STARTS[ch], STARTS[ch] + WIDTHS[ch]
        received(st.at[:, pl.ds(0, NX - 1), :, cols(ch)], st_r.at[ch])
        if ch == LAST:
            return
        part = modes_back(zh[:, lo:hi], zl[:, lo:hi], ch)
        if ch == 0:
            ba[...] = part
        else:
            ba[...] += part

    def blocks(g):
        return [(k, o, (core(o) * NZ + zmod(k)) * 64) for k in GROUPS[g] for o in range(NC)]

    def over_y(g):
        lo, hi = STARTS[LAST], STARTS[LAST] + WIDTHS[LAST]

        def rows(ref, a, b):
            return jnp.concatenate(
                [ref[pl.ds(pl.multiple_of(at, 64), 64), a:b] for _, _, at in blocks(g)], axis=0
            )

        total = rows(ba, 0, 128) + modes_back(rows(zh, lo, hi), rows(zl, lo, hi), LAST)
        for n in range(4):
            pieces = swap_blocks([total[64 * n + 16 * m : 64 * n + 16 * (m + 1)] for m in range(4)])
            for p in range(NY):
                bp[p, g, n] = pieces[p]
        for k in (2, 1, 3):
            yy = ymod(k)
            send(bp.at[yy, g], br.at[k - 1, g], by_s, by_r.at[g], {"y": yy})

    def leave(g):
        received(br.at[:, g], by_r.at[g])
        op[g] = bp[y, g] + br[0, g] + br[1, g] + br[2, g]
        for n, (k, o, _) in enumerate(blocks(g)):
            if k == 0 and o == 0:
                orr[2 * z + c] = op[g, n]
            else:
                send(op.at[g, n], orr.at[2 * z + c], oz_s, oz_r.at[g], {"z": zmod(k), "c": core(o)})

    def last(g):
        received(orr.at[pl.ds(0, 3 if g == 3 else 4)], oz_r.at[g])
        near = [zmod(-k) for k in GROUPS[g]]
        parts = swap_blocks([orr[2 * zz + cc] for zz in near for cc in range(NC)])
        high, low = halves(jnp.concatenate(parts, axis=0))

        def rows(ref):
            return jnp.concatenate([ref[pl.ds(pl.multiple_of(64 * zz, 64), 64), :] for zz in near], axis=0)

        both = dot(jnp.concatenate([high, low], axis=0), rows(yth))
        part = both[:64] + both[64:] + dot(high, rows(ytl))
        out[...] = part if g == 0 else out[...] + part

    def drain():
        sent(zg.at[0, pl.ds(0, NZ - 1)], zs_s)
        sent(zg.at[0], zd_s)
        sent(fp.at[pl.ds(0, 15)], fa_s)
        sent(fg.at[pl.ds(0, NY - 1)], fy_s)
        sent(cr, cs_s)
        sent(st.at[:, pl.ds(0, NX - 1)], st_s)
        sent(br, by_s)
        sent(orr.at[pl.ds(0, 15)], oz_s)

    plan = [
        (start,), (meet,),
        (own, 0), (own, 1), (own, 4), (along_y,), (meet_far,), (a2a,), (prepare,), (arr, 1, 0), (arr, 1, 1),
        (own, 2), (arr, 1, 4), (arr, 2, 0), (fy,), (arr, 2, 1), (own, 5), (own, 3), (arr, 1, 2), (arr, 2, 4),
        (arr, 3, 0), (arr, 3, 1), (arr, 1, 5), (arr, 1, 3), (arr, 2, 2), (ft,), (arr, 3, 4), (arr, 4, 0),
        (arr, 4, 1), (C, 0), (arr, 2, 5), (C, 1), (arr, 2, 3), (arr, 3, 2), (arr, 4, 4), (arr, 3, 5), (C, 4),
        (arr, 3, 3), (S, 0), (arr, 4, 2), (S, 1), (arr, 4, 5), (C, 2), (arr, 4, 3), (C, 5), (C, 3), (S, 4),
        (B, 0), (B, 1), (S, 2), (S, 5), (S, 3), (B, 4), (B, 2), (B, 5), (B, 3),
        (over_y, 0), (over_y, 1), (over_y, 2), (over_y, 3),
        (leave, 0), (leave, 1), (leave, 2), (leave, 3),
        (last, 0), (last, 1), (last, 2), (last, 3), (drain,),
    ]
    for step, *args in plan:
        with jax.named_scope("_".join([step.__name__, *map(str, args)])):
            step(*args)


def shards(source, z_vectors, x_vectors, y_vectors, z_values, x_values, y_values):
    f32, bf16 = jnp.float32, jnp.bfloat16
    vmem, smem, dma = pltpu.VMEM, pltpu.SMEM, pltpu.SemaphoreType.DMA
    modes = z_vectors.shape[1]
    one = dma(())
    told = pltpu.SemaphoreType.REGULAR
    return pl.pallas_call(
        kernel,
        out_shape=jax.ShapeDtypeStruct(source.shape, f32),
        in_specs=[pl.BlockSpec(memory_space=pltpu.HBM)] * 7,
        out_specs=pl.BlockSpec(memory_space=pltpu.VMEM),
        scratch_shapes=[
            vmem(source.shape, f32),
            vmem(z_vectors.shape, f32),
            vmem(y_vectors.shape, f32),
            vmem((1, z_values.shape[0]), f32),
            smem(x_vectors.shape, f32),
            smem(x_values.shape, f32),
            smem(y_values.shape, f32),
            dma((7,)),
            vmem((NC, NZ, 64, modes), f32),
            vmem((1024, modes), bf16),
            vmem((1024, modes), bf16),
            vmem((512, 512), bf16),
            vmem((512, 512), bf16),
            vmem((16, 16, 128), f32),
            vmem((NY, NC, NZ, 16, 128), f32),
            vmem((256, 1024), bf16),
            vmem((4, NX, 8, modes), f32),
            vmem((NX - 1, 4, 8, modes), f32),
            vmem((4, NX, 8, modes), f32),
            vmem((1024, 128), f32),
            vmem((NY, 4, 4, 16, 128), f32),
            vmem((NY - 1, 4, 4, 16, 128), f32),
            vmem((4, 4, 16, 128), f32),
            vmem((16, 16, 128), f32),
            one, dma((4, N)), one, dma((N,)), one, one, one, one,
            one, dma((N,)), one, dma((N,)), one, dma((4,)), one, dma((4,)),
            told((2, 3)), told(()), told(()), told(()),
        ],
        compiler_params=pltpu.CompilerParams(
            collective_id=0, has_side_effects=True, vmem_limit_bytes=32 * 1024 * 1024
        ),
    )(*[
        pltpu.with_memory_space_constraint(a, pltpu.HBM)
        for a in (source, z_vectors, y_vectors, z_values.reshape(1, -1), x_vectors, x_values, y_values)
    ])


def solution(mesh):
    torus = Mesh(mesh.devices.reshape(NZ, NX, NC, NY), ("z", "x", "c", "y"))
    rows = ("z", "x", "c")
    return jax.shard_map(
        shards,
        mesh=torus,
        in_specs=(P(rows, "y"), P(rows, "y"), P(), P(), P(), P(), P()),
        out_specs=P(rows, "y"),
        check_vma=False,
    )
```

```python
import jax
import jax.numpy as jnp
from jax import lax
from jax.experimental import pallas as pl
from jax.experimental.pallas import tpu as pltpu
from jax.sharding import Mesh
from jax.sharding import PartitionSpec as P

NZ, NX, NC, NY = 8, 4, 2, 4
MESH = pl.DeviceIdType.MESH
WIDTHS = (128, 128, 128, 128, 128, 128, 128, 128)
N = len(WIDTHS)
FIRST, LAST = 0, 2
STARTS = tuple(sum(WIDTHS[:ch]) for ch in range(N))
FAR_FIRST = (4, 3, 5, 2, 6, 1, 7, 0)


def dot_exact(a, b):
    return lax.dot_general(
        a, b, (((1,), (0,)), ((), ())),
        precision=lax.Precision.HIGHEST, preferred_element_type=jnp.float32,
    )


def dot(a, b, b_dim=0):
    return lax.dot_general(a, b, (((1,), (b_dim,)), ((), ())), preferred_element_type=jnp.float32)


def halves(value):
    high = value.astype(jnp.bfloat16)
    return high, (value - high.astype(jnp.float32)).astype(jnp.bfloat16)


def swap_blocks(parts):
    shape = parts[0].shape
    block = lax.broadcasted_iota(jnp.int32, shape, 1) // 32
    out = []
    for q in range(4):
        total = None
        for m in range(4):
            shift = 32 * ((m - q) % 4)
            moved = parts[m] if shift == 0 else pltpu.roll(parts[m], shift, 1)
            total = moved if total is None else jnp.where(block == m, moved, total)
        out.append(total)
    return out


def kernel(
    src_h, zv_h, yv_h, zval_h, xv_h, xval_h, yval_h, out,
    src, zv, yv, zval, xv, xval, yval, in_s,
    zg, zh, zl, yth, ytl, fp, fg, fts, cs, cr, st, ba, bp, br, op, orr,
    zs_s, zs_r, zd_s, zd_r, fa_s, fa_r, fy_s, fy_r,
    cs_s, cs_r, st_s, st_r, by_s, by_r, oz_s, oz_r, zi, xi, yi, pi,
):
    z = lax.axis_index("z")
    x = lax.axis_index("x")
    c = lax.axis_index("c")
    y = lax.axis_index("y")
    pc = 1 - c

    def send(src_ref, dst_ref, s_sem, r_sem, dev):
        pltpu.make_async_remote_copy(
            src_ref=src_ref, dst_ref=dst_ref, send_sem=s_sem, recv_sem=r_sem,
            device_id=dev, device_id_type=MESH,
        ).start()

    def sized(ref, sem):
        return pltpu.make_async_remote_copy(
            src_ref=ref, dst_ref=ref, send_sem=sem, recv_sem=sem,
            device_id={"c": pc}, device_id_type=MESH,
        )

    def received(ref, sem):
        sized(ref, sem).wait_recv()

    def sent(ref, sem):
        sized(ref, sem).wait_send()

    def zmod(k):
        return lax.rem(z + k + NZ, NZ)

    def xmod(k):
        return lax.rem(x + k + NX, NX)

    def ymod(k):
        return lax.rem(y + k + NY, NY)

    def tell(sem, dev):
        pl.semaphore_signal(sem, inc=1, device_id=dev, device_id_type=MESH)

    def core(o):
        return c if o == 0 else pc

    def cols(ch):
        return pl.ds(STARTS[ch], WIDTHS[ch])

    def load(n):
        pairs = [(zv_h, zv), (src_h, src), (yv_h, yv), (zval_h, zval), (xv_h, xv), (xval_h, xval), (yval_h, yval)]
        return pltpu.make_async_copy(*pairs[n], in_s.at[n])

    def start():
        load(0).start()
        for way in (1, -1):
            for dev in ({"z": zmod(way)}, {"z": zmod(way), "c": pc}, {"x": xmod(way)}, {"y": ymod(way)}):
                tell(pltpu.get_barrier_semaphore(), dev)
        tell(pltpu.get_barrier_semaphore(), {"c": pc})
        for n in range(1, 7):
            load(n).start()

    def along_y():
        load(1).wait()
        load(2).wait()
        along = dot_exact(src[...], yv[...])
        for g in range(4):
            v = along[:, 128 * g : 128 * (g + 1)]
            pieces = swap_blocks([v[16 * m : 16 * (m + 1)] for m in range(4)])
            for q in range(4):
                fp[4 * g + q] = pieces[q]
        fg[y, c, z] = fp[2 * z + c]

    def meet():
        load(0).wait()
        pl.semaphore_wait(pltpu.get_barrier_semaphore(), 9)
        tell(zi.at[0, 0], {"z": zmod(1)})
        tell(zi.at[1, 0], {"z": zmod(-1)})
        tell(xi, {"x": xmod(-1)})
        tell(yi, {"y": ymod(-1)})

    def meet_second():
        pl.semaphore_wait(zi.at[0, 0], 1)
        pl.semaphore_wait(zi.at[1, 0], 1)
        tell(zi.at[0, 1], {"z": zmod(2)})
        tell(zi.at[1, 1], {"z": zmod(-2)})

    def meet_far():
        pl.semaphore_wait(zi.at[0, 1], 1)
        pl.semaphore_wait(zi.at[1, 1], 1)
        pl.semaphore_wait(xi, 1)
        pl.semaphore_wait(yi, 1)

    def pass_on(ch, s, way):
        slot = zmod(-s * way)
        block = zv.at[:, cols(ch)] if s == 0 else zg.at[c, slot, :, cols(ch)]
        if s < NZ // 2 - 1 or (s == NZ // 2 - 1 and (ch % 2 == 0) == (way == 1)):
            send(block, zg.at[c, slot, :, cols(ch)], zs_s, zs_r.at[s, ch], {"z": zmod(way)})
        if s > 0 or way == 1:
            send(block, zg.at[c, slot, :, cols(ch)], zd_s, zd_r.at[ch], {"c": pc})

    def own(ch):
        pass_on(ch, 0, 1)
        pass_on(ch, 0, -1)

    def arr(s, ch):
        ways = (1, -1) if s < NZ // 2 else ((1,) if ch % 2 == 0 else (-1,))
        received(zg.at[c, pl.ds(0, len(ways)), :, cols(ch)], zs_r.at[s - 1, ch])
        for way in ways:
            pass_on(ch, s, way)

    def prepare():
        zg[c, z] = zv[...]
        for n in range(3, 7):
            load(n).wait()
        high, low = halves(yv[...].T)
        yth[...] = high
        ytl[...] = low

    def a2(part):
        if part == 0:
            along_y()
        if part == 1:
            meet_second()
        if part == 2:
            meet_far()
        for k in ((1, -1), (2, -2), (4, 3, -3))[part]:
            for o in range(NC):
                dev = {"z": zmod(k), "c": core(o)}
                send(fp.at[2 * zmod(k) + core(o)], fg.at[y, c, z], fa_s, fa_r.at[part // 2], dev)
        if part == 0:
            send(fp.at[2 * z + pc], fg.at[y, c, z], fa_s, fa_r.at[0], {"c": pc})

    def fy(part):
        received(fp.at[pl.ds(0, 9 if part == 0 else 6)], fa_r.at[part])
        for k in (2, 1, 3):
            for d in ((0, 1, -1, 2, -2), (3, -3, 4))[part]:
                piece = fg.at[y, :, zmod(d)]
                send(piece, piece, fy_s, fy_r, {"y": ymod(k)})

    def ft():
        received(fg.at[pl.ds(0, NY - 1)], fy_r)
        for pair in range(NC * NZ // 2):
            rows = []
            for b in (2 * pair, 2 * pair + 1):
                rows += swap_blocks([fg[p, b // NZ, b % NZ] for p in range(NY)])
            high, low = halves(jnp.concatenate(rows, axis=0).T)
            fts[0:128, 128 * pair : 128 * (pair + 1)] = high
            fts[128:256, 128 * pair : 128 * (pair + 1)] = low

    def C(ch):
        lo, hi = STARTS[ch], STARTS[ch] + WIDTHS[ch]
        received(zg.at[pc, :, :, cols(ch)], zd_r.at[ch])
        high, low = halves(zg[:, :, :, lo:hi].reshape(NC * NZ * 64, WIDTHS[ch]))
        zh[:, lo:hi] = high
        zl[:, lo:hi] = low
        both = dot(fts[...], high)
        part = both[:128] + both[128:] + dot(fts[:128], low)
        cs[:, :, :, lo:hi] = part.reshape(4, NX, 8, WIDTHS[ch])
        for k in (2, 1, 3):
            xx = xmod(k)
            send(cs.at[:, xx, :, cols(ch)], cr.at[k - 1, :, :, cols(ch)], cs_s, cs_r.at[ch], {"x": xx})

    def S(ch):
        lo, hi = STARTS[ch], STARTS[ch] + WIDTHS[ch]
        received(cr.at[:, :, :, cols(ch)], cs_r.at[ch])
        base = (2 * z + c) * 32 + 8 * x
        row = lax.broadcasted_iota(jnp.int32, (8, WIDTHS[ch]), 0)
        yvals = jnp.zeros((8, WIDTHS[ch]), jnp.float32)
        for t in range(8):
            yvals = jnp.where(row == t, yval[base + t], yvals)
        zy = yvals + zval[:, pl.ds(pl.multiple_of(y * zv.shape[1] + lo, 128), WIDTHS[ch])]
        total = [
            cs[p, x, :, lo:hi] + cr[0, p, :, lo:hi] + cr[1, p, :, lo:hi] + cr[2, p, :, lo:hi] for p in range(4)
        ]
        scaled = []
        for i in range(4):
            mode = xv[0, i] * total[0]
            for p in range(1, 4):
                mode = mode + xv[p, i] * total[p]
            scaled.append(mode / (zy + xval[i]))
        for p in range(4):
            back = xv[p, 0] * scaled[0]
            for i in range(1, 4):
                back = back + xv[p, i] * scaled[i]
            st[p, x, :, lo:hi] = back
        for k in (2, 1, 3):
            piece = st.at[:, x, :, cols(ch)]
            send(piece, piece, st_s, st_r.at[ch], {"x": xmod(k)})

    def modes_back(high, low, ch):
        lo, hi = STARTS[ch], STARTS[ch] + WIDTHS[ch]
        s_high, s_low = halves(st[:, :, :, lo:hi].reshape(128, WIDTHS[ch]))
        both = dot(high, jnp.concatenate([s_high, s_low], axis=0), 1)
        return both[:, :128] + both[:, 128:] + dot(low, s_high, 1)

    def B(ch):
        lo, hi = STARTS[ch], STARTS[ch] + WIDTHS[ch]
        received(st.at[:, pl.ds(0, NX - 1), :, cols(ch)], st_r.at[ch])
        if ch == LAST:
            return
        part = modes_back(zh[:, lo:hi], zl[:, lo:hi], ch)
        if ch == FIRST:
            ba[...] = part
        else:
            ba[...] += part

    def blocks(g):
        return [(k, o, (core(o) * NZ + zmod(k)) * 64) for k in FAR_FIRST[2 * g : 2 * g + 2] for o in range(NC)]

    def over_y(g):
        lo, hi = STARTS[LAST], STARTS[LAST] + WIDTHS[LAST]

        def rows(ref, a, b):
            return jnp.concatenate(
                [ref[pl.ds(pl.multiple_of(at, 64), 64), a:b] for _, _, at in blocks(g)], axis=0
            )

        total = rows(ba, 0, 128) + modes_back(rows(zh, lo, hi), rows(zl, lo, hi), LAST)
        for n in range(4):
            pieces = swap_blocks([total[64 * n + 16 * m : 64 * n + 16 * (m + 1)] for m in range(4)])
            for p in range(NY):
                bp[p, g, n] = pieces[p]
        for k in (2, 1, 3):
            yy = ymod(k)
            send(bp.at[yy, g], br.at[k - 1, g], by_s, by_r.at[g], {"y": yy})

    def leave(g):
        received(br.at[:, g], by_r.at[g])
        op[g] = bp[y, g] + br[0, g] + br[1, g] + br[2, g]
        for n, (k, o, _) in enumerate(blocks(g)):
            if k == 0 and o == 0:
                orr[2 * z + c] = op[g, n]
            else:
                send(op.at[g, n], orr.at[2 * z + c], oz_s, oz_r.at[g], {"z": zmod(k), "c": core(o)})

    def last(g):
        received(orr.at[pl.ds(0, 3 if g == 3 else 4)], oz_r.at[g])
        near = [zmod(-k) for k in FAR_FIRST[2 * g : 2 * g + 2]]
        parts = swap_blocks([orr[2 * zz + cc] for zz in near for cc in range(NC)])
        high, low = halves(jnp.concatenate(parts, axis=0))

        def rows(ref):
            return jnp.concatenate([ref[pl.ds(pl.multiple_of(64 * zz, 64), 64), :] for zz in near], axis=0)

        both = dot(jnp.concatenate([high, low], axis=0), rows(yth))
        part = both[:64] + both[64:] + dot(high, rows(ytl))
        out[...] = part if g == 0 else out[...] + part

    def drain():
        sent(zg.at[0, pl.ds(0, NZ - 1)], zs_s)
        sent(zg.at[0], zd_s)
        sent(fp.at[pl.ds(0, 15)], fa_s)
        sent(fg.at[pl.ds(0, NY - 1)], fy_s)
        sent(cr, cs_s)
        sent(st.at[:, pl.ds(0, NX - 1)], st_s)
        sent(br, by_s)
        sent(orr.at[pl.ds(0, 15)], oz_s)

    plan = [
        (start,), (meet,),
        (own, 0), (own, 3), (a2, 0), (a2, 1), (own, 5), (arr, 1, 0), (a2, 2), (prepare,), (arr, 1, 3),
        (fy, 0), (arr, 1, 5), (arr, 2, 0), (own, 6), (own, 1), (arr, 2, 3), (own, 7), (arr, 2, 5), (own, 4),
        (own, 2), (arr, 3, 0), (fy, 1), (arr, 1, 6), (arr, 1, 1), (arr, 3, 3), (arr, 1, 7), (arr, 3, 5),
        (arr, 1, 4), (arr, 1, 2), (ft,), (arr, 4, 0), (arr, 2, 6), (arr, 2, 1), (arr, 4, 3), (C, 0),
        (arr, 2, 7), (C, 3), (arr, 4, 5), (arr, 2, 4), (arr, 2, 2), (C, 5), (arr, 3, 6), (arr, 3, 1), (S, 0),
        (arr, 3, 7), (S, 3), (arr, 3, 4), (arr, 3, 2), (arr, 4, 6), (S, 5), (arr, 4, 1), (C, 6), (arr, 4, 7),
        (C, 1), (arr, 4, 4), (C, 7), (arr, 4, 2), (C, 4), (C, 2), (B, 0), (S, 6), (S, 1), (S, 7), (S, 4),
        (S, 2), (B, 3), (B, 5), (B, 6), (B, 1), (B, 7), (B, 4), (B, 2),
        *((over_y, g) for g in range(4)), *((leave, g) for g in range(4)),
        (last, 0), (last, 1), (last, 2), (last, 3), (drain,),
    ]
    for step, *args in plan:
        with jax.named_scope("_".join([step.__name__, *map(str, args)])):
            step(*args)


def shards(source, z_vectors, x_vectors, y_vectors, z_values, x_values, y_values):
    f32, bf16 = jnp.float32, jnp.bfloat16
    vmem, smem, dma = pltpu.VMEM, pltpu.SMEM, pltpu.SemaphoreType.DMA
    modes = z_vectors.shape[1]
    one = dma(())
    told = pltpu.SemaphoreType.REGULAR
    return pl.pallas_call(
        kernel,
        out_shape=jax.ShapeDtypeStruct(source.shape, f32),
        in_specs=[pl.BlockSpec(memory_space=pltpu.HBM)] * 7,
        out_specs=pl.BlockSpec(memory_space=pltpu.VMEM),
        scratch_shapes=[
            vmem(source.shape, f32),
            vmem(z_vectors.shape, f32),
            vmem(y_vectors.shape, f32),
            vmem((1, z_values.shape[0]), f32),
            smem(x_vectors.shape, f32),
            smem(x_values.shape, f32),
            smem(y_values.shape, f32),
            dma((7,)),
            vmem((NC, NZ, 64, modes), f32),
            vmem((1024, modes), bf16),
            vmem((1024, modes), bf16),
            vmem((512, 512), bf16),
            vmem((512, 512), bf16),
            vmem((16, 16, 128), f32),
            vmem((NY, NC, NZ, 16, 128), f32),
            vmem((256, 1024), bf16),
            vmem((4, NX, 8, modes), f32),
            vmem((NX - 1, 4, 8, modes), f32),
            vmem((4, NX, 8, modes), f32),
            vmem((1024, 128), f32),
            vmem((NY, 4, 4, 16, 128), f32),
            vmem((NY - 1, 4, 4, 16, 128), f32),
            vmem((4, 4, 16, 128), f32),
            vmem((16, 16, 128), f32),
            one, dma((4, N)), one, dma((N,)), one, dma((2,)), one, one,
            one, dma((N,)), one, dma((N,)), one, dma((4,)), one, dma((4,)),
            told((2, 2)), told(()), told(()), told(()),
        ],
        compiler_params=pltpu.CompilerParams(
            collective_id=0, has_side_effects=True, vmem_limit_bytes=32 * 1024 * 1024
        ),
    )(*[
        pltpu.with_memory_space_constraint(a, pltpu.HBM)
        for a in (source, z_vectors, y_vectors, z_values.reshape(1, -1), x_vectors, x_values, y_values)
    ])


def solution(mesh):
    torus = Mesh(mesh.devices.reshape(NZ, NX, NC, NY), ("z", "x", "c", "y"))
    rows = ("z", "x", "c")
    return jax.shard_map(
        shards,
        mesh=torus,
        in_specs=(P(rows, "y"), P(rows, "y"), P(), P(), P(), P(), P()),
        out_specs=P(rows, "y"),
        check_vma=False,
    )
```

```python
import jax
import jax.numpy as jnp
from jax import lax
from jax.experimental import pallas as pl
from jax.experimental.pallas import tpu as pltpu
from jax.sharding import Mesh
from jax.sharding import PartitionSpec as P

NZ, NX, NC, NY = 8, 4, 2, 4
MESH = pl.DeviceIdType.MESH
WIDTHS = (128, 128, 128, 128, 128, 128, 128, 128)
N = len(WIDTHS)
FIRST, LAST = 0, 2
STARTS = tuple(sum(WIDTHS[:ch]) for ch in range(N))
FAR_FIRST = (4, 3, 5, 2, 6, 1, 7, 0)


def dot_exact(a, b):
    return lax.dot_general(
        a, b, (((1,), (0,)), ((), ())),
        precision=lax.Precision.HIGHEST, preferred_element_type=jnp.float32,
    )


def dot(a, b, b_dim=0):
    return lax.dot_general(a, b, (((1,), (b_dim,)), ((), ())), preferred_element_type=jnp.float32)


def halves(value):
    high = value.astype(jnp.bfloat16)
    return high, (value - high.astype(jnp.float32)).astype(jnp.bfloat16)


def swap_blocks(parts):
    shape = parts[0].shape
    block = lax.broadcasted_iota(jnp.int32, shape, 1) // 32
    out = []
    for q in range(4):
        total = None
        for m in range(4):
            shift = 32 * ((m - q) % 4)
            moved = parts[m] if shift == 0 else pltpu.roll(parts[m], shift, 1)
            total = moved if total is None else jnp.where(block == m, moved, total)
        out.append(total)
    return out


def kernel(
    src_h, zv_h, yv_h, zval_h, xv_h, xval_h, yval_h, out,
    src, zv, yv, zval, xv, xval, yval, in_s,
    zg, zh, zl, yth, ytl, fp, fg, fts, cs, cr, st, ba, bp, br, op, orr,
    zs_s, zs_r, zd_s, zd_r, fa_s, fa_r, fy_s, fy_r,
    cs_s, cs_r, st_s, st_r, by_s, by_r, oz_s, oz_r, zi, xi, yi, pi,
):
    z = lax.axis_index("z")
    x = lax.axis_index("x")
    c = lax.axis_index("c")
    y = lax.axis_index("y")
    pc = 1 - c

    def send(src_ref, dst_ref, s_sem, r_sem, dev):
        pltpu.make_async_remote_copy(
            src_ref=src_ref, dst_ref=dst_ref, send_sem=s_sem, recv_sem=r_sem,
            device_id=dev, device_id_type=MESH,
        ).start()

    def sized(ref, sem):
        return pltpu.make_async_remote_copy(
            src_ref=ref, dst_ref=ref, send_sem=sem, recv_sem=sem,
            device_id={"c": pc}, device_id_type=MESH,
        )

    def received(ref, sem):
        sized(ref, sem).wait_recv()

    def sent(ref, sem):
        sized(ref, sem).wait_send()

    def zmod(k):
        return lax.rem(z + k + NZ, NZ)

    def xmod(k):
        return lax.rem(x + k + NX, NX)

    def ymod(k):
        return lax.rem(y + k + NY, NY)

    def tell(sem, dev):
        pl.semaphore_signal(sem, inc=1, device_id=dev, device_id_type=MESH)

    def core(o):
        return c if o == 0 else pc

    def cols(ch):
        return pl.ds(STARTS[ch], WIDTHS[ch])

    def load(n):
        pairs = [(zv_h, zv), (src_h, src), (yv_h, yv), (zval_h, zval), (xv_h, xv), (xval_h, xval), (yval_h, yval)]
        return pltpu.make_async_copy(*pairs[n], in_s.at[n])

    def start():
        load(0).start()
        for way in (1, -1):
            for dev in ({"z": zmod(way)}, {"z": zmod(way), "c": pc}, {"x": xmod(way)}, {"y": ymod(way)}):
                tell(pltpu.get_barrier_semaphore(), dev)
        tell(pltpu.get_barrier_semaphore(), {"c": pc})
        for n in range(1, 7):
            load(n).start()

    def along_y():
        load(1).wait()
        load(2).wait()
        along = dot_exact(src[...], yv[...])
        for g in range(4):
            v = along[:, 128 * g : 128 * (g + 1)]
            pieces = swap_blocks([v[16 * m : 16 * (m + 1)] for m in range(4)])
            for q in range(4):
                fp[4 * g + q] = pieces[q]
        fg[y, c, z] = fp[2 * z + c]

    def meet():
        load(0).wait()
        pl.semaphore_wait(pltpu.get_barrier_semaphore(), 9)
        tell(zi.at[0, 0], {"z": zmod(1)})
        tell(zi.at[1, 0], {"z": zmod(-1)})
        tell(xi, {"x": xmod(-1)})
        tell(yi, {"y": ymod(-1)})

    def meet_second():
        pl.semaphore_wait(zi.at[0, 0], 1)
        pl.semaphore_wait(zi.at[1, 0], 1)
        tell(zi.at[0, 1], {"z": zmod(2)})
        tell(zi.at[1, 1], {"z": zmod(-2)})

    def meet_far():
        pl.semaphore_wait(zi.at[0, 1], 1)
        pl.semaphore_wait(zi.at[1, 1], 1)
        pl.semaphore_wait(xi, 1)
        pl.semaphore_wait(yi, 1)

    def pass_on(ch, s, way):
        slot = zmod(-s * way)
        block = zv.at[:, cols(ch)] if s == 0 else zg.at[c, slot, :, cols(ch)]
        if s < NZ // 2 - 1 or (s == NZ // 2 - 1 and (ch % 2 == 0) == (way == 1)):
            send(block, zg.at[c, slot, :, cols(ch)], zs_s, zs_r.at[s, ch], {"z": zmod(way)})
        if s > 0 or way == 1:
            send(block, zg.at[c, slot, :, cols(ch)], zd_s, zd_r.at[ch], {"c": pc})

    def own(ch):
        pass_on(ch, 0, 1)
        pass_on(ch, 0, -1)

    def arr(s, ch):
        ways = (1, -1) if s < NZ // 2 else ((1,) if ch % 2 == 0 else (-1,))
        received(zg.at[c, pl.ds(0, len(ways)), :, cols(ch)], zs_r.at[s - 1, ch])
        for way in ways:
            pass_on(ch, s, way)

    def prepare():
        zg[c, z] = zv[...]
        for n in range(3, 7):
            load(n).wait()
        high, low = halves(yv[...].T)
        yth[...] = high
        ytl[...] = low

    def a2(part):
        if part == 0:
            along_y()
        if part == 1:
            meet_second()
        if part == 2:
            meet_far()
        for k in ((1, -1), (2, -2), (4, 3, -3))[part]:
            for o in range(NC):
                dev = {"z": zmod(k), "c": core(o)}
                send(fp.at[2 * zmod(k) + core(o)], fg.at[y, c, z], fa_s, fa_r.at[part // 2], dev)
        if part == 0:
            send(fp.at[2 * z + pc], fg.at[y, c, z], fa_s, fa_r.at[0], {"c": pc})

    def fy(part):
        received(fp.at[pl.ds(0, 9 if part == 0 else 6)], fa_r.at[part])
        for k in (2, 1, 3):
            for d in ((0, 1, -1, 2, -2), (3, -3, 4))[part]:
                piece = fg.at[y, :, zmod(d)]
                send(piece, piece, fy_s, fy_r, {"y": ymod(k)})

    def ft():
        received(fg.at[pl.ds(0, NY - 1)], fy_r)
        for pair in range(NC * NZ // 2):
            rows = []
            for b in (2 * pair, 2 * pair + 1):
                rows += swap_blocks([fg[p, b // NZ, b % NZ] for p in range(NY)])
            high, low = halves(jnp.concatenate(rows, axis=0).T)
            fts[0:128, 128 * pair : 128 * (pair + 1)] = high
            fts[128:256, 128 * pair : 128 * (pair + 1)] = low

    def C(ch):
        lo, hi = STARTS[ch], STARTS[ch] + WIDTHS[ch]
        received(zg.at[pc, :, :, cols(ch)], zd_r.at[ch])
        high, low = halves(zg[:, :, :, lo:hi].reshape(NC * NZ * 64, WIDTHS[ch]))
        zh[:, lo:hi] = high
        zl[:, lo:hi] = low
        both = dot(fts[...], high)
        part = both[:128] + both[128:] + dot(fts[:128], low)
        cs[:, :, :, lo:hi] = part.reshape(4, NX, 8, WIDTHS[ch])
        for k in (2, 1, 3):
            xx = xmod(k)
            send(cs.at[:, xx, :, cols(ch)], cr.at[k - 1, :, :, cols(ch)], cs_s, cs_r.at[ch], {"x": xx})

    def S(ch):
        lo, hi = STARTS[ch], STARTS[ch] + WIDTHS[ch]
        received(cr.at[:, :, :, cols(ch)], cs_r.at[ch])
        base = (2 * z + c) * 32 + 8 * x
        row = lax.broadcasted_iota(jnp.int32, (8, WIDTHS[ch]), 0)
        yvals = jnp.zeros((8, WIDTHS[ch]), jnp.float32)
        for t in range(8):
            yvals = jnp.where(row == t, yval[base + t], yvals)
        zy = yvals + zval[:, pl.ds(pl.multiple_of(y * zv.shape[1] + lo, 128), WIDTHS[ch])]
        total = [
            cs[p, x, :, lo:hi] + cr[0, p, :, lo:hi] + cr[1, p, :, lo:hi] + cr[2, p, :, lo:hi] for p in range(4)
        ]
        scaled = []
        for i in range(4):
            mode = xv[0, i] * total[0]
            for p in range(1, 4):
                mode = mode + xv[p, i] * total[p]
            scaled.append(mode / (zy + xval[i]))
        for p in range(4):
            back = xv[p, 0] * scaled[0]
            for i in range(1, 4):
                back = back + xv[p, i] * scaled[i]
            st[p, x, :, lo:hi] = back
        for k in (2, 1, 3):
            piece = st.at[:, x, :, cols(ch)]
            send(piece, piece, st_s, st_r.at[ch], {"x": xmod(k)})

    def modes_back(high, low, ch):
        lo, hi = STARTS[ch], STARTS[ch] + WIDTHS[ch]
        s_high, s_low = halves(st[:, :, :, lo:hi].reshape(128, WIDTHS[ch]))
        both = dot(high, jnp.concatenate([s_high, s_low], axis=0), 1)
        return both[:, :128] + both[:, 128:] + dot(low, s_high, 1)

    def B(ch):
        lo, hi = STARTS[ch], STARTS[ch] + WIDTHS[ch]
        received(st.at[:, pl.ds(0, NX - 1), :, cols(ch)], st_r.at[ch])
        if ch == LAST:
            return
        part = modes_back(zh[:, lo:hi], zl[:, lo:hi], ch)
        if ch == FIRST:
            ba[...] = part
        else:
            ba[...] += part

    def blocks(g):
        return [(k, o, (core(o) * NZ + zmod(k)) * 64) for k in FAR_FIRST[2 * g : 2 * g + 2] for o in range(NC)]

    def over_y(g):
        lo, hi = STARTS[LAST], STARTS[LAST] + WIDTHS[LAST]

        def rows(ref, a, b):
            return jnp.concatenate(
                [ref[pl.ds(pl.multiple_of(at, 64), 64), a:b] for _, _, at in blocks(g)], axis=0
            )

        total = rows(ba, 0, 128) + modes_back(rows(zh, lo, hi), rows(zl, lo, hi), LAST)
        for n in range(4):
            pieces = swap_blocks([total[64 * n + 16 * m : 64 * n + 16 * (m + 1)] for m in range(4)])
            for p in range(NY):
                bp[p, g, n] = pieces[p]
        for k in (2, 1, 3):
            yy = ymod(k)
            send(bp.at[yy, g], br.at[k - 1, g], by_s, by_r.at[g], {"y": yy})

    def leave(g):
        received(br.at[:, g], by_r.at[g])
        op[g] = bp[y, g] + br[0, g] + br[1, g] + br[2, g]
        for n, (k, o, _) in enumerate(blocks(g)):
            if k == 0 and o == 0:
                orr[2 * z + c] = op[g, n]
            else:
                send(op.at[g, n], orr.at[2 * z + c], oz_s, oz_r.at[g], {"z": zmod(k), "c": core(o)})

    def last(g):
        received(orr.at[pl.ds(0, 3 if g == 3 else 4)], oz_r.at[g])
        near = [zmod(-k) for k in FAR_FIRST[2 * g : 2 * g + 2]]
        parts = swap_blocks([orr[2 * zz + cc] for zz in near for cc in range(NC)])
        high, low = halves(jnp.concatenate(parts, axis=0))

        def rows(ref):
            return jnp.concatenate([ref[pl.ds(pl.multiple_of(64 * zz, 64), 64), :] for zz in near], axis=0)

        both = dot(jnp.concatenate([high, low], axis=0), rows(yth))
        part = both[:64] + both[64:] + dot(high, rows(ytl))
        out[...] = part if g == 0 else out[...] + part

    def drain():
        sent(zg.at[0, pl.ds(0, NZ - 1)], zs_s)
        sent(zg.at[0], zd_s)
        sent(fp.at[pl.ds(0, 15)], fa_s)
        sent(fg.at[pl.ds(0, NY - 1)], fy_s)
        sent(cr, cs_s)
        sent(st.at[:, pl.ds(0, NX - 1)], st_s)
        sent(br, by_s)
        sent(orr.at[pl.ds(0, 15)], oz_s)

    plan = [
        (start,), (meet,),
        (own, 0), (own, 3), (a2, 0), (a2, 1), (own, 5), (arr, 1, 0), (a2, 2), (prepare,), (arr, 1, 3),
        (fy, 0), (arr, 1, 5), (arr, 2, 0), (own, 6), (own, 1), (arr, 2, 3), (own, 7), (arr, 2, 5), (own, 4),
        (own, 2), (arr, 3, 0), (fy, 1), (arr, 1, 6), (arr, 1, 1), (arr, 3, 3), (arr, 1, 7), (arr, 3, 5),
        (arr, 1, 4), (arr, 1, 2), (ft,), (arr, 4, 0), (arr, 2, 6), (arr, 2, 1), (arr, 4, 3), (C, 0),
        (arr, 2, 7), (C, 3), (arr, 4, 5), (arr, 2, 4), (arr, 2, 2), (C, 5), (arr, 3, 6), (arr, 3, 1),
        (arr, 3, 7),  (arr, 3, 4), (arr, 3, 2), (S, 0), (S, 3), (S, 5), (arr, 4, 6),  (arr, 4, 1), (C, 6), (arr, 4, 7),
        (C, 1), (arr, 4, 4), (C, 7), (arr, 4, 2), (C, 4), (C, 2), (B, 0), (S, 6), (S, 1), (S, 7), (S, 4),
        (S, 2), (B, 3), (B, 5), (B, 6), (B, 1), (B, 7), (B, 4), (B, 2),
        *((over_y, g) for g in range(4)), *((leave, g) for g in range(4)),
        (last, 0), (last, 1), (last, 2), (last, 3), (drain,),
    ]
    for step, *args in plan:
        with jax.named_scope("_".join([step.__name__, *map(str, args)])):
            step(*args)


def shards(source, z_vectors, x_vectors, y_vectors, z_values, x_values, y_values):
    f32, bf16 = jnp.float32, jnp.bfloat16
    vmem, smem, dma = pltpu.VMEM, pltpu.SMEM, pltpu.SemaphoreType.DMA
    modes = z_vectors.shape[1]
    one = dma(())
    told = pltpu.SemaphoreType.REGULAR
    return pl.pallas_call(
        kernel,
        out_shape=jax.ShapeDtypeStruct(source.shape, f32),
        in_specs=[pl.BlockSpec(memory_space=pltpu.HBM)] * 7,
        out_specs=pl.BlockSpec(memory_space=pltpu.VMEM),
        scratch_shapes=[
            vmem(source.shape, f32),
            vmem(z_vectors.shape, f32),
            vmem(y_vectors.shape, f32),
            vmem((1, z_values.shape[0]), f32),
            smem(x_vectors.shape, f32),
            smem(x_values.shape, f32),
            smem(y_values.shape, f32),
            dma((7,)),
            vmem((NC, NZ, 64, modes), f32),
            vmem((1024, modes), bf16),
            vmem((1024, modes), bf16),
            vmem((512, 512), bf16),
            vmem((512, 512), bf16),
            vmem((16, 16, 128), f32),
            vmem((NY, NC, NZ, 16, 128), f32),
            vmem((256, 1024), bf16),
            vmem((4, NX, 8, modes), f32),
            vmem((NX - 1, 4, 8, modes), f32),
            vmem((4, NX, 8, modes), f32),
            vmem((1024, 128), f32),
            vmem((NY, 4, 4, 16, 128), f32),
            vmem((NY - 1, 4, 4, 16, 128), f32),
            vmem((4, 4, 16, 128), f32),
            vmem((16, 16, 128), f32),
            one, dma((4, N)), one, dma((N,)), one, dma((2,)), one, one,
            one, dma((N,)), one, dma((N,)), one, dma((4,)), one, dma((4,)),
            told((2, 2)), told(()), told(()), told(()),
        ],
        compiler_params=pltpu.CompilerParams(
            collective_id=0, has_side_effects=True, vmem_limit_bytes=32 * 1024 * 1024
        ),
    )(*[
        pltpu.with_memory_space_constraint(a, pltpu.HBM)
        for a in (source, z_vectors, y_vectors, z_values.reshape(1, -1), x_vectors, x_values, y_values)
    ])


def solution(mesh):
    torus = Mesh(mesh.devices.reshape(NZ, NX, NC, NY), ("z", "x", "c", "y"))
    rows = ("z", "x", "c")
    return jax.shard_map(
        shards,
        mesh=torus,
        in_specs=(P(rows, "y"), P(rows, "y"), P(), P(), P(), P(), P()),
        out_specs=P(rows, "y"),
        check_vma=False,
    )
```
